32 devices in a mesh: zero: 8 (over z, x), tp: 4 (over y, core).
Axes of the slice: x: 2, y: 2, z: 4, core: 2. Of those that a mesh axis runs over, the one named last changes fastest.
Arguments:
- train_gate: float32 [2048, 8192], P('zero', 'tp'), may hold values from -0.1875 to 0.1875
- slow_gate: float32 [2048, 8192], P('zero', 'tp'), may hold values from -0.125 to 0.125
- train_up: float32 [2048, 8192], P('zero', 'tp'), may hold values from -0.1875 to 0.1875
- slow_up: float32 [2048, 8192], P('zero', 'tp'), may hold values from -0.125 to 0.125
- norm_gain: float32 [2048], P('zero'), may hold values from 0.25 to 1.75
Outputs:
- serving_gate: bfloat16 [2048, 8192], P(None, 'tp')
- serving_up: bfloat16 [2048, 8192], P(None, 'tp')
- scale_gate: float32 [8192], P('tp')
- scale_up: float32 [8192], P('tp')
The draws below stay inside these ranges and needn't reach their ends.
All inputs are finite; a program needn't handle non-finite values.
Results may differ from the reference program's by a relative error of at most 0.0004.
Values may be sent and summed in bfloat16 or wider, within the bound.
A program may use at most 128 MiB of HBM per device.

```python
import jax
import jax.numpy as jnp
from jax import lax

D_MODEL = 2048
D_INNER = 8192


def spiked(drawn, key, source, target, shards_of, factor):
    def block_of(axis_at):
        return (jnp.arange(drawn.shape[axis_at]) // (drawn.shape[axis_at] // shards_of)).reshape((-1,) + (1,) * (drawn.ndim - 1 - axis_at))

    near = jax.random.permutation(key, shards_of)[block_of(target)]
    second = (block_of(target) + shards_of // 2) % shards_of
    return jnp.where((block_of(source) == near) | (block_of(source) == second), factor * drawn, drawn)


def block_scale(own_key, dims, split, least, largest):
    gain, own = 1.0, jax.random.fold_in(own_key, 6)
    for dim, parts in split:
        draws = jnp.exp(jax.random.uniform(jax.random.fold_in(own, dim), (parts,), jnp.float32, least / len(split), largest / len(split)))
        gain = gain * jnp.repeat(draws, dims[dim] // parts).reshape([-1 if axis == dim else 1 for axis in range(len(dims))])
    return gain


def gaussian(rng, shape, scale, most, cuts=(), held_as=jnp.bfloat16):
    factor_of = block_scale(rng, shape, cuts, -0.22, 0.18) if cuts else 1.0
    array = jax.random.normal(rng, shape, jnp.float32) * scale * factor_of
    return jnp.minimum(jnp.maximum(array, -most), most).astype(held_as)


def gaussian_with(stream_key, dims, width, bound, pieces, heavy, held_as=jnp.bfloat16):
    array = width * jax.random.normal(stream_key, dims, jnp.float32)
    if pieces:
        array = array * block_scale(stream_key, dims, pieces, -0.22, 0.18)
    return jnp.clip(spiked(array, jax.random.fold_in(stream_key, 3), *heavy), -bound, bound).astype(held_as)


def setup_inputs(seed: int = 0) -> dict:
    arg_keys = jax.random.split(jax.random.key(seed), 6)
    train_gate = gaussian_with(arg_keys[0], (D_MODEL, D_INNER), D_MODEL ** -0.5, 0.1875, ((0, 8), (1, 4)), (0, 1, 8, 2.0), jnp.float32)
    slow_gate = gaussian(arg_keys[1], (D_MODEL, D_INNER), D_MODEL ** -0.5, 0.125, ((0, 8), (1, 4)), jnp.float32)
    train_up = gaussian_with(arg_keys[2], (D_MODEL, D_INNER), D_MODEL ** -0.5, 0.1875, ((0, 8), (1, 4)), (0, 1, 8, 2.0), jnp.float32)
    slow_up = gaussian(arg_keys[3], (D_MODEL, D_INNER), D_MODEL ** -0.5, 0.125, ((0, 8), (1, 4)), jnp.float32)
    norm_gain = jnp.clip(1.0 + 0.15 * jax.random.normal(arg_keys[4], (D_MODEL,), jnp.float32), 0.25, 1.75)
    return {"train_gate": train_gate, "slow_gate": slow_gate, "train_up": train_up, "slow_up": slow_up, "norm_gain": norm_gain}


keep_rate = 0.75

def reference(train_gate, slow_gate, train_up, slow_up, norm_gain):
    whole_gate = keep_rate * slow_gate + (1.0 - keep_rate) * train_gate
    whole_up = keep_rate * slow_up + (1.0 - keep_rate) * train_up
    whole_gained_gate = whole_gate * norm_gain[:, None]
    whole_gained_up = whole_up * norm_gain[:, None]
    scale_gate = jnp.sqrt(lax.optimization_barrier(jnp.sum(whole_gained_gate * whole_gained_gate, axis=0)))
    serving_gate = (whole_gained_gate / scale_gate).astype(jnp.bfloat16)
    scale_up = jnp.sqrt(lax.optimization_barrier(jnp.sum(whole_gained_up * whole_gained_up, axis=0)))
    serving_up = (whole_gained_up / scale_up).astype(jnp.bfloat16)
    return (serving_gate, serving_up, scale_gate, scale_up)
```

```python
import functools

import jax
import jax.numpy as jnp
from jax import lax
from jax.experimental import pallas as pl
from jax.experimental.pallas import tpu as pltpu
from jax.sharding import PartitionSpec as P

keep_rate = 0.75
MESH = pl.DeviceIdType.MESH
SIDE = 2


def gather_kernel(
    count, pieces,
    train_gate, slow_gate, train_up, slow_up, gain_ref,
    gate_ref, up_ref, scale_gate_ref, scale_up_ref,
    train, slow, sums,
    load_sem, sum_send, sum_recv,
    left_send, left_recv, right_send, right_recv, side_send, side_recv, half_send, half_recv,
):
    length = count // SIDE
    rows = train_gate.shape[0]
    piece_rows = rows // pieces
    me = lax.axis_index("zero")
    place, side = me // SIDE, me % SIDE
    outs = (gate_ref, up_ref)

    loads = []
    for which, (t, s) in enumerate(((train_gate, slow_gate), (train_up, slow_up))):
        for p in range(pieces):
            at = pl.ds(p * piece_rows, piece_rows)
            k = (which * pieces + p) * 2
            loads.append((
                pltpu.make_async_copy(t.at[at], train.at[which, at], load_sem.at[k]),
                pltpu.make_async_copy(s.at[at], slow.at[which, at], load_sem.at[k + 1]),
            ))
    for pair in loads:
        for load in pair:
            load.start()

    barrier = pltpu.get_barrier_semaphore()
    for step in range(1, count):
        pl.semaphore_signal(barrier, 1, device_id={"zero": lax.rem(me + step, count)}, device_id_type=MESH)

    for which in range(2):
        total = None
        for p in range(pieces):
            for load in loads[which * pieces + p]:
                load.wait()
            at = pl.ds(p * piece_rows, piece_rows)
            gained = (keep_rate * slow[which, at, :] + (1.0 - keep_rate) * train[which, at, :]) * gain_ref[at, :]
            slow[which, at, :] = gained
            part = jnp.sum(gained * gained, axis=0, keepdims=True)
            total = part if total is None else total + part
        sums[me, pl.ds(which, 1), :] = total

    pl.semaphore_wait(barrier, count - 1)
    sum_copies = []
    for step in range(1, count):
        copy = pltpu.make_async_remote_copy(
            src_ref=sums.at[me], dst_ref=sums.at[me],
            send_sem=sum_send.at[step - 1], recv_sem=sum_recv.at[step - 1],
            device_id={"zero": lax.rem(me + step, count)}, device_id_type=MESH,
        )
        copy.start()
        sum_copies.append(copy)
    for step in range(1, count):
        source = lax.rem(me + count - step, count)
        pltpu.make_async_remote_copy(
            src_ref=sums.at[source], dst_ref=sums.at[source],
            send_sem=sum_send.at[step - 1], recv_sem=sum_recv.at[step - 1],
            device_id={"zero": source}, device_id_type=MESH,
        ).wait_recv()
    total = sums[0]
    for k in range(1, count):
        total = total + sums[k]
    scale = jnp.sqrt(total)
    scale_gate_ref[...] = scale[0:1]
    scale_up_ref[...] = scale[1:2]
    inverse = 1.0 / scale

    def part_of(owner_place, owner_side, which, p):
        start = (owner_place * SIDE + owner_side) * rows + p * piece_rows
        return outs[which].at[pl.ds(pl.multiple_of(start, piece_rows), piece_rows)]

    def copy_to(ref, send, recv, to):
        return pltpu.make_async_remote_copy(
            src_ref=ref, dst_ref=ref, send_sem=send, recv_sem=recv,
            device_id={"zero": to}, device_id_type=MESH,
        )

    to_left = jnp.maximum(place - 1, 0) * SIDE + side
    to_right = jnp.minimum(place + 1, length - 1) * SIDE + side
    to_side = place * SIDE + (SIDE - 1 - side)
    has_left, has_right = place > 0, place < length - 1
    is_even = place % 2 == 0
    twin = place + 1 - 2 * (place % 2)
    to_twin = twin * SIDE + side
    order = [(which, p) for which in range(2) for p in range(pieces)]

    def left_copy(distance, which, p):
        k = distance * 2 * pieces + which * pieces + p
        return copy_to(part_of(place + distance, side, which, p), left_send.at[k], left_recv.at[k], to_left)

    def right_copy(distance, which, p):
        k = distance * 2 * pieces + which * pieces + p
        return copy_to(part_of(place - distance, side, which, p), right_send.at[k], right_recv.at[k], to_right)

    def side_index(distance, which, p):
        d = distance if distance >= 0 else length - 1 - distance
        return d * 2 * pieces + which * pieces + p

    def side_copy(distance, which, p):
        k = side_index(distance, which, p)
        return copy_to(part_of(place + distance, side, which, p), side_send.at[k], side_recv.at[k], to_side)

    def side_arrival(distance, which, p):
        k = side_index(distance, which, p)
        return copy_to(part_of(place + distance, SIDE - 1 - side, which, p), side_send.at[k], side_recv.at[k], to_side)

    def half_copy(p):
        return copy_to(part_of(place, SIDE - 1 - side, 1, p), half_send.at[p], half_recv.at[p], to_twin)

    def half_arrival(p):
        return copy_to(part_of(twin, SIDE - 1 - side, 1, p), half_send.at[p], half_recv.at[p], to_twin)

    def in_line(distance):
        return place + distance <= length - 1 if distance > 0 else place + distance >= 0

    def by_side(distance, which):
        ok = in_line(distance)
        if which == 1 and distance == 1:
            ok = jnp.logical_and(ok, jnp.logical_not(is_even))
        if which == 1 and distance == -1:
            ok = jnp.logical_and(ok, is_even)
        return ok

    def send_own(which, p):
        @pl.when(has_left)
        def _():
            left_copy(0, which, p).start()

        @pl.when(has_right)
        def _():
            right_copy(0, which, p).start()

        side_copy(0, which, p).start()

    previous = None
    for which, p in order:
        at = pl.ds(p * piece_rows, piece_rows)
        start = pl.multiple_of(me * rows + p * piece_rows, piece_rows)
        outs[which][pl.ds(start, piece_rows), :] = (slow[which, at, :] * inverse[which:which + 1]).astype(jnp.bfloat16)
        if previous is not None:
            send_own(*previous)
        previous = (which, p)
    send_own(*previous)

    for k in range(1, length):
        for which, p in order:
            @pl.when(in_line(k))
            def _():
                q = (k - 1) * 2 * pieces + which * pieces + p
                copy_to(part_of(place + k, side, which, p), left_send.at[q], left_recv.at[q], to_right).wait_recv()

                @pl.when(has_left)
                def _():
                    left_copy(k, which, p).start()

            @pl.when(by_side(k, which))
            def _():
                side_copy(k, which, p).start()

            @pl.when(in_line(-k))
            def _():
                q = (k - 1) * 2 * pieces + which * pieces + p
                copy_to(part_of(place - k, side, which, p), right_send.at[q], right_recv.at[q], to_left).wait_recv()

                @pl.when(has_right)
                def _():
                    right_copy(k, which, p).start()

            @pl.when(by_side(-k, which))
            def _():
                side_copy(-k, which, p).start()

    for which, p in order:
        side_arrival(0, which, p).wait_recv()
        if which == 1:
            half_copy(p).start()

    for k in range(1, length):
        for which, p in order:
            for distance in (k, -k):
                @pl.when(by_side(distance, which))
                def _():
                    side_arrival(distance, which, p).wait_recv()
                    side_copy(distance, which, p).wait_send()

    for p in range(pieces):
        half_arrival(p).wait_recv()
        half_copy(p).wait_send()

    for copy in sum_copies:
        copy.wait_send()
    for which, p in order:
        side_copy(0, which, p).wait_send()
        for k in range(length):
            @pl.when(jnp.logical_and(has_left, place + k <= length - 1))
            def _():
                left_copy(k, which, p).wait_send()

            @pl.when(jnp.logical_and(has_right, place - k >= 0))
            def _():
                right_copy(k, which, p).wait_send()


def solution(mesh):
    count = mesh.shape["zero"]

    def body(train_gate, slow_gate, train_up, slow_up, norm_gain):
        rows, columns = train_gate.shape
        pieces = max(1, min(4, rows // 64))
        length = count // SIDE
        block = pltpu.VMEM((rows * count, columns), jnp.bfloat16)
        scale = jax.ShapeDtypeStruct((1, columns), jnp.float32)
        vmem, held = pl.BlockSpec(memory_space=pltpu.VMEM), pl.BlockSpec(memory_space=pltpu.HBM)
        dma = lambda n: pltpu.SemaphoreType.DMA((n,))
        line, wide = length * 2 * pieces, (2 * length - 1) * 2 * pieces
        gate, up, scale_gate, scale_up = pl.pallas_call(
            functools.partial(gather_kernel, count, pieces),
            out_shape=(block, block, scale, scale),
            in_specs=[held] * 4 + [vmem],
            out_specs=(vmem,) * 4,
            scratch_shapes=[
                pltpu.VMEM((2, rows, columns), jnp.float32),
                pltpu.VMEM((2, rows, columns), jnp.float32),
                pltpu.VMEM((count, 2, columns), jnp.float32),
                dma(4 * pieces), dma(count - 1), dma(count - 1),
                dma(line), dma(line), dma(line), dma(line), dma(wide), dma(wide), dma(pieces), dma(pieces),
            ],
            compiler_params=pltpu.CompilerParams(
                collective_id=0, has_side_effects=True, vmem_limit_bytes=24 << 20
            ),
        )(train_gate, slow_gate, train_up, slow_up, norm_gain[:, None])
        return gate, up, scale_gate[0], scale_up[0]

    in_specs = (P("zero", "tp"), P("zero", "tp"), P("zero", "tp"), P("zero", "tp"), P("zero"))
    out_specs = (P(None, "tp"), P(None, "tp"), P("tp"), P("tp"))
    return jax.shard_map(body, mesh=mesh, in_specs=in_specs, out_specs=out_specs, check_vma=False)
```

```python
import functools

import jax
import jax.numpy as jnp
from jax import lax
from jax.experimental import pallas as pl
from jax.experimental.pallas import tpu as pltpu
from jax.sharding import PartitionSpec as P

keep_rate = 0.75
MESH = pl.DeviceIdType.MESH
SIDE = 2
LANES = 128
GROUP = 8
VMEM_BYTES = 67_043_328


def gather_kernel(
    count, pieces,
    train_gate, slow_gate, train_up, slow_up, gain_ref,
    gate_ref, up_ref, scale_gate_ref, scale_up_ref,
    train, slow, gains, sums,
    load_sem, sum_send, sum_recv,
    left_send, left_recv, right_send, right_recv, side_send, side_recv, half_send, half_recv,
):
    length = count // SIDE
    rows, columns = train_gate.shape
    piece_rows = rows // pieces
    me = lax.axis_index("zero")
    place, side = me // SIDE, me % SIDE
    outs = (gate_ref, up_ref)
    scales = (scale_gate_ref, scale_up_ref)

    loads = []
    for which, (t, s) in enumerate(((train_gate, slow_gate), (train_up, slow_up))):
        for p in range(pieces):
            at = pl.ds(p * piece_rows, piece_rows)
            k = (which * pieces + p) * 2
            loads.append((
                pltpu.make_async_copy(t.at[at], train.at[which, at], load_sem.at[k]),
                pltpu.make_async_copy(s.at[at], slow.at[which, at], load_sem.at[k + 1]),
            ))
    for pair in loads:
        for load in pair:
            load.start()

    barrier = pltpu.get_barrier_semaphore()
    for step in range(1, count):
        pl.semaphore_signal(barrier, 1, device_id={"zero": lax.rem(me + step, count)}, device_id_type=MESH)

    gains[...] = jnp.broadcast_to(gain_ref[...], (LANES, rows)).T

    def sum_copy(which, step, source, to):
        k = which * (count - 1) + step - 1
        return pltpu.make_async_remote_copy(
            src_ref=sums.at[which, source], dst_ref=sums.at[which, source],
            send_sem=sum_send.at[k], recv_sem=sum_recv.at[k],
            device_id={"zero": to}, device_id_type=MESH,
        )

    for which in range(2):
        def add(i, total):
            at = pl.ds(pl.multiple_of(i * GROUP, GROUP), GROUP)
            gain = jnp.concatenate([gains[at, :]] * (columns // LANES), axis=1)
            gained = (keep_rate * slow[which, at, :] + (1.0 - keep_rate) * train[which, at, :]) * gain
            slow[which, at, :] = gained
            return total + gained * gained

        total = jnp.zeros((GROUP, columns), jnp.float32)
        for p in range(pieces):
            for load in loads[which * pieces + p]:
                load.wait()
            total = lax.fori_loop(p * piece_rows // GROUP, (p + 1) * piece_rows // GROUP, add, total)
        sums[which, me] = jnp.sum(total, axis=0, keepdims=True)
        if which == 0:
            pl.semaphore_wait(barrier, count - 1)
        for step in range(1, count):
            sum_copy(which, step, me, lax.rem(me + step, count)).start()

    def part_of(owner_place, owner_side, which, p):
        start = (owner_place * SIDE + owner_side) * rows + p * piece_rows
        return outs[which].at[pl.ds(pl.multiple_of(start, piece_rows), piece_rows)]

    def copy_to(ref, send, recv, to):
        return pltpu.make_async_remote_copy(
            src_ref=ref, dst_ref=ref, send_sem=send, recv_sem=recv,
            device_id={"zero": to}, device_id_type=MESH,
        )

    to_left = jnp.maximum(place - 1, 0) * SIDE + side
    to_right = jnp.minimum(place + 1, length - 1) * SIDE + side
    to_side = place * SIDE + (SIDE - 1 - side)
    has_left, has_right = place > 0, place < length - 1
    is_even = place % 2 == 0
    twin = place + 1 - 2 * (place % 2)
    to_twin = twin * SIDE + side
    order = [(which, p) for which in range(2) for p in range(pieces)]

    def left_copy(distance, which, p):
        k = distance * 2 * pieces + which * pieces + p
        return copy_to(part_of(place + distance, side, which, p), left_send.at[k], left_recv.at[k], to_left)

    def right_copy(distance, which, p):
        k = distance * 2 * pieces + which * pieces + p
        return copy_to(part_of(place - distance, side, which, p), right_send.at[k], right_recv.at[k], to_right)

    def side_index(distance, which, p):
        d = distance if distance >= 0 else length - 1 - distance
        return d * 2 * pieces + which * pieces + p

    def side_copy(distance, which, p):
        k = side_index(distance, which, p)
        return copy_to(part_of(place + distance, side, which, p), side_send.at[k], side_recv.at[k], to_side)

    def side_arrival(distance, which, p):
        k = side_index(distance, which, p)
        return copy_to(part_of(place + distance, SIDE - 1 - side, which, p), side_send.at[k], side_recv.at[k], to_side)

    def half_copy(p):
        return copy_to(part_of(place, SIDE - 1 - side, 1, p), half_send.at[p], half_recv.at[p], to_twin)

    def half_arrival(p):
        return copy_to(part_of(twin, SIDE - 1 - side, 1, p), half_send.at[p], half_recv.at[p], to_twin)

    def in_line(distance):
        return place + distance <= length - 1 if distance > 0 else place + distance >= 0

    def by_side(distance, which):
        ok = in_line(distance)
        if which == 1 and distance == 1:
            ok = jnp.logical_and(ok, jnp.logical_not(is_even))
        if which == 1 and distance == -1:
            ok = jnp.logical_and(ok, is_even)
        return ok

    def send_own(which, p):
        @pl.when(has_left)
        def _():
            left_copy(0, which, p).start()

        @pl.when(has_right)
        def _():
            right_copy(0, which, p).start()

        side_copy(0, which, p).start()

    for which in range(2):
        for step in range(1, count):
            source = lax.rem(me + count - step, count)
            sum_copy(which, step, source, source).wait_recv()
        total = sums[which, 0]
        for k in range(1, count):
            total = total + sums[which, k]
        scale = jnp.sqrt(total)
        scales[which][...] = scale
        inverse = 1.0 / scale
        for p in range(pieces + 1):
            if p < pieces:
                at = pl.ds(p * piece_rows, piece_rows)
                start = pl.multiple_of(me * rows + p * piece_rows, piece_rows)
                outs[which][pl.ds(start, piece_rows), :] = (slow[which, at, :] * inverse).astype(jnp.bfloat16)
            if p > 0:
                send_own(which, p - 1)

    for k in range(1, length):
        for which, p in order:
            @pl.when(in_line(k))
            def _():
                q = (k - 1) * 2 * pieces + which * pieces + p
                copy_to(part_of(place + k, side, which, p), left_send.at[q], left_recv.at[q], to_right).wait_recv()

                @pl.when(has_left)
                def _():
                    left_copy(k, which, p).start()

            @pl.when(by_side(k, which))
            def _():
                side_copy(k, which, p).start()

            @pl.when(in_line(-k))
            def _():
                q = (k - 1) * 2 * pieces + which * pieces + p
                copy_to(part_of(place - k, side, which, p), right_send.at[q], right_recv.at[q], to_left).wait_recv()

                @pl.when(has_right)
                def _():
                    right_copy(k, which, p).start()

            @pl.when(by_side(-k, which))
            def _():
                side_copy(-k, which, p).start()

    for which, p in order:
        side_arrival(0, which, p).wait_recv()
        if which == 1:
            half_copy(p).start()

    for k in range(1, length):
        for which, p in order:
            for distance in (k, -k):
                @pl.when(by_side(distance, which))
                def _():
                    side_arrival(distance, which, p).wait_recv()
                    side_copy(distance, which, p).wait_send()

    for p in range(pieces):
        half_arrival(p).wait_recv()
        half_copy(p).wait_send()

    for which in range(2):
        for step in range(1, count):
            sum_copy(which, step, me, lax.rem(me + step, count)).wait_send()
    for which, p in order:
        side_copy(0, which, p).wait_send()
        for k in range(length):
            @pl.when(jnp.logical_and(has_left, place + k <= length - 1))
            def _():
                left_copy(k, which, p).wait_send()

            @pl.when(jnp.logical_and(has_right, place - k >= 0))
            def _():
                right_copy(k, which, p).wait_send()


def store_kernel(parts, gate, up, scale_gate, scale_up, gate_out, up_out, scale_gate_out, scale_up_out, sem):
    rows = gate.shape[0] // parts
    copies = []
    for which, (held, out) in enumerate(((gate, gate_out), (up, up_out))):
        for k in range(parts):
            at = pl.ds(k * rows, rows)
            copies.append(pltpu.make_async_copy(held.at[at], out.at[at], sem.at[which * parts + k]))
    for copy in copies:
        copy.start()
    scale_gate_out[...] = scale_gate[0, :]
    scale_up_out[...] = scale_up[0, :]
    for copy in copies:
        copy.wait()


def solution(mesh):
    count = mesh.shape["zero"]

    def body(train_gate, slow_gate, train_up, slow_up, norm_gain):
        rows, columns = train_gate.shape
        pieces = max(1, min(4, rows // 64))
        length = count // SIDE
        full = (rows * count, columns)
        block = pltpu.VMEM(full, jnp.bfloat16)
        scale = pltpu.VMEM((1, columns), jnp.float32)
        vmem, held = pl.BlockSpec(memory_space=pltpu.VMEM), pl.BlockSpec(memory_space=pltpu.HBM)
        dma = lambda n: pltpu.SemaphoreType.DMA((n,))
        line, wide = length * 2 * pieces, (2 * length - 1) * 2 * pieces
        gathered = pl.pallas_call(
            functools.partial(gather_kernel, count, pieces),
            out_shape=(block, block, scale, scale),
            in_specs=[held] * 4 + [vmem],
            out_specs=(vmem,) * 4,
            scratch_shapes=[
                pltpu.VMEM((2, rows, columns), jnp.float32),
                pltpu.VMEM((2, rows, columns), jnp.float32),
                pltpu.VMEM((rows, LANES), jnp.float32),
                pltpu.VMEM((2, count, 1, columns), jnp.float32),
                dma(4 * pieces), dma(2 * count - 2), dma(2 * count - 2),
                dma(line), dma(line), dma(line), dma(line), dma(wide), dma(wide), dma(pieces), dma(pieces),
            ],
            compiler_params=pltpu.CompilerParams(
                collective_id=0, has_side_effects=True,
                vmem_limit_bytes=VMEM_BYTES - 2 * full[0] * full[1] * 2 - (1 << 19),
            ),
        )(train_gate, slow_gate, train_up, slow_up, norm_gain[None, :])
        parts = 8
        return pl.pallas_call(
            functools.partial(store_kernel, parts),
            out_shape=(jax.ShapeDtypeStruct(full, jnp.bfloat16),) * 2 + (jax.ShapeDtypeStruct((columns,), jnp.float32),) * 2,
            in_specs=[vmem] * 4,
            out_specs=(held, held, vmem, vmem),
            scratch_shapes=[dma(2 * parts)],
            compiler_params=pltpu.CompilerParams(vmem_limit_bytes=1 << 20),
        )(*gathered)

    in_specs = (P("zero", "tp"), P("zero", "tp"), P("zero", "tp"), P("zero", "tp"), P("zero"))
    out_specs = (P(None, "tp"), P(None, "tp"), P("tp"), P("tp"))
    return jax.shard_map(body, mesh=mesh, in_specs=in_specs, out_specs=out_specs, check_vma=False)
```

```python
import functools

import jax
import jax.numpy as jnp
from jax import lax
from jax.experimental import pallas as pl
from jax.experimental.pallas import tpu as pltpu
from jax.sharding import PartitionSpec as P

keep_rate = 0.75
MESH = pl.DeviceIdType.MESH
SIDE = 2
LANES = 128
GROUP = 8
VMEM_BYTES = 67_043_328


def gather_kernel(
    count, pieces,
    train_gate, slow_gate, train_up, slow_up, gain_ref,
    gate_ref, up_ref, scale_gate_ref, scale_up_ref,
    train, slow, gains, sums,
    load_sem, sum_send, sum_recv,
    left_send, left_recv, right_send, right_recv, side_send, side_recv, half_send, half_recv,
):
    length = count // SIDE
    rows, columns = train_gate.shape
    piece_rows = rows // pieces
    me = lax.axis_index("zero")
    place, side = me // SIDE, me % SIDE
    outs = (gate_ref, up_ref)
    scales = (scale_gate_ref, scale_up_ref)

    barrier = pltpu.get_barrier_semaphore()
    for step in range(1, count):
        pl.semaphore_signal(barrier, 1, device_id={"zero": lax.rem(me + step, count)}, device_id_type=MESH)

    loads = []
    for which, (t, s) in enumerate(((train_gate, slow_gate), (train_up, slow_up))):
        for p in range(pieces):
            at = pl.ds(p * piece_rows, piece_rows)
            k = (which * pieces + p) * 2
            loads.append((
                pltpu.make_async_copy(t.at[at], train.at[which, at], load_sem.at[k]),
                pltpu.make_async_copy(s.at[at], slow.at[which, at], load_sem.at[k + 1]),
            ))
    for pair in loads:
        for load in pair:
            load.start()

    gains[...] = jnp.broadcast_to(gain_ref[...], (LANES, rows)).T

    def sum_copy(which, step, source, to):
        k = which * (count - 1) + step - 1
        return pltpu.make_async_remote_copy(
            src_ref=sums.at[which, source], dst_ref=sums.at[which, source],
            send_sem=sum_send.at[k], recv_sem=sum_recv.at[k],
            device_id={"zero": to}, device_id_type=MESH,
        )

    for which in range(2):
        def add(i, total):
            at = pl.ds(pl.multiple_of(i * GROUP, GROUP), GROUP)
            gain = jnp.concatenate([gains[at, :]] * (columns // LANES), axis=1)
            gained = (keep_rate * slow[which, at, :] + (1.0 - keep_rate) * train[which, at, :]) * gain
            slow[which, at, :] = gained
            return total + gained * gained

        total = jnp.zeros((GROUP, columns), jnp.float32)
        for p in range(pieces):
            for load in loads[which * pieces + p]:
                load.wait()
            total = lax.fori_loop(p * piece_rows // GROUP, (p + 1) * piece_rows // GROUP, add, total)
        sums[which, me] = jnp.sum(total, axis=0, keepdims=True)
        if which == 0:
            pl.semaphore_wait(barrier, count - 1)
        for step in range(1, count):
            sum_copy(which, step, me, lax.rem(me + step, count)).start()

    def part_of(owner_place, owner_side, which, p):
        start = (owner_place * SIDE + owner_side) * rows + p * piece_rows
        return outs[which].at[pl.ds(pl.multiple_of(start, piece_rows), piece_rows)]

    def copy_to(ref, send, recv, to):
        return pltpu.make_async_remote_copy(
            src_ref=ref, dst_ref=ref, send_sem=send, recv_sem=recv,
            device_id={"zero": to}, device_id_type=MESH,
        )

    to_left = jnp.maximum(place - 1, 0) * SIDE + side
    to_right = jnp.minimum(place + 1, length - 1) * SIDE + side
    to_side = place * SIDE + (SIDE - 1 - side)
    has_left, has_right = place > 0, place < length - 1
    is_even = place % 2 == 0
    twin = place + 1 - 2 * (place % 2)
    to_twin = twin * SIDE + side
    half_round = jnp.maximum(jnp.where(is_even, place, length - 1 - place), 1)
    order = [(which, p) for which in range(2) for p in range(pieces)]

    def left_copy(distance, which, p):
        k = distance * 2 * pieces + which * pieces + p
        return copy_to(part_of(place + distance, side, which, p), left_send.at[k], left_recv.at[k], to_left)

    def right_copy(distance, which, p):
        k = distance * 2 * pieces + which * pieces + p
        return copy_to(part_of(place - distance, side, which, p), right_send.at[k], right_recv.at[k], to_right)

    def side_index(distance, which, p):
        d = distance if distance >= 0 else length - 1 - distance
        return d * 2 * pieces + which * pieces + p

    def side_copy(distance, which, p):
        k = side_index(distance, which, p)
        return copy_to(part_of(place + distance, side, which, p), side_send.at[k], side_recv.at[k], to_side)

    def side_arrival(distance, which, p):
        k = side_index(distance, which, p)
        return copy_to(part_of(place + distance, SIDE - 1 - side, which, p), side_send.at[k], side_recv.at[k], to_side)

    def half_copy(p):
        return copy_to(part_of(place, SIDE - 1 - side, 1, p), half_send.at[p], half_recv.at[p], to_twin)

    def half_arrival(p):
        return copy_to(part_of(twin, SIDE - 1 - side, 1, p), half_send.at[p], half_recv.at[p], to_twin)

    def in_line(distance):
        return place + distance <= length - 1 if distance > 0 else place + distance >= 0

    def by_side(distance, which):
        ok = in_line(distance)
        if which == 1 and distance == 1:
            ok = jnp.logical_and(ok, jnp.logical_not(is_even))
        if which == 1 and distance == -1:
            ok = jnp.logical_and(ok, is_even)
        return ok

    def send_own(which, p):
        @pl.when(has_left)
        def _():
            left_copy(0, which, p).start()

        @pl.when(has_right)
        def _():
            right_copy(0, which, p).start()

        side_copy(0, which, p).start()

    for which in range(2):
        for step in range(1, count):
            source = lax.rem(me + count - step, count)
            sum_copy(which, step, source, source).wait_recv()
        total = sums[which, 0]
        for k in range(1, count):
            total = total + sums[which, k]
        scale = jnp.sqrt(total)
        scales[which][...] = scale
        inverse = 1.0 / scale
        for p in range(pieces + 1):
            if p < pieces:
                at = pl.ds(p * piece_rows, piece_rows)
                start = pl.multiple_of(me * rows + p * piece_rows, piece_rows)
                outs[which][pl.ds(start, piece_rows), :] = (slow[which, at, :] * inverse).astype(jnp.bfloat16)
            if p > 0:
                send_own(which, p - 1)

    for k in range(1, length):
        for which, p in order:
            @pl.when(in_line(k))
            def _():
                q = (k - 1) * 2 * pieces + which * pieces + p
                copy_to(part_of(place + k, side, which, p), left_send.at[q], left_recv.at[q], to_right).wait_recv()

                @pl.when(has_left)
                def _():
                    left_copy(k, which, p).start()

            @pl.when(by_side(k, which))
            def _():
                side_copy(k, which, p).start()

            @pl.when(in_line(-k))
            def _():
                q = (k - 1) * 2 * pieces + which * pieces + p
                copy_to(part_of(place - k, side, which, p), right_send.at[q], right_recv.at[q], to_left).wait_recv()

                @pl.when(has_right)
                def _():
                    right_copy(k, which, p).start()

            @pl.when(by_side(-k, which))
            def _():
                side_copy(-k, which, p).start()

        @pl.when(half_round == k)
        def _():
            for p in range(pieces):
                side_arrival(0, 1, p).wait_recv()
                half_copy(p).start()

    for p in range(pieces):
        side_arrival(0, 0, p).wait_recv()

    for k in range(1, length):
        for which, p in order:
            for distance in (k, -k):
                @pl.when(by_side(distance, which))
                def _():
                    side_arrival(distance, which, p).wait_recv()
                    side_copy(distance, which, p).wait_send()

    for p in range(pieces):
        half_arrival(p).wait_recv()
        half_copy(p).wait_send()

    for which in range(2):
        for step in range(1, count):
            sum_copy(which, step, me, lax.rem(me + step, count)).wait_send()
    for which, p in order:
        side_copy(0, which, p).wait_send()
        for k in range(length):
            @pl.when(jnp.logical_and(has_left, place + k <= length - 1))
            def _():
                left_copy(k, which, p).wait_send()

            @pl.when(jnp.logical_and(has_right, place - k >= 0))
            def _():
                right_copy(k, which, p).wait_send()


def store_kernel(parts, gate, up, scale_gate, scale_up, gate_out, up_out, scale_gate_out, scale_up_out, sem):
    rows = gate.shape[0] // parts
    copies = []
    for which, (held, out) in enumerate(((gate, gate_out), (up, up_out))):
        for k in range(parts):
            at = pl.ds(k * rows, rows)
            copies.append(pltpu.make_async_copy(held.at[at], out.at[at], sem.at[which * parts + k]))
    copies.append(pltpu.make_async_copy(scale_gate.at[0], scale_gate_out, sem.at[2 * parts]))
    copies.append(pltpu.make_async_copy(scale_up.at[0], scale_up_out, sem.at[2 * parts + 1]))
    for copy in copies:
        copy.start()
    for copy in copies:
        copy.wait()


def solution(mesh):
    count = mesh.shape["zero"]

    def body(train_gate, slow_gate, train_up, slow_up, norm_gain):
        rows, columns = train_gate.shape
        pieces = max(1, min(4, rows // 64))
        length = count // SIDE
        full = (rows * count, columns)
        block = pltpu.VMEM(full, jnp.bfloat16)
        scale = pltpu.VMEM((1, columns), jnp.float32)
        vmem, held = pl.BlockSpec(memory_space=pltpu.VMEM), pl.BlockSpec(memory_space=pltpu.HBM)
        dma = lambda n: pltpu.SemaphoreType.DMA((n,))
        line, wide = length * 2 * pieces, (2 * length - 1) * 2 * pieces
        gathered = pl.pallas_call(
            functools.partial(gather_kernel, count, pieces),
            out_shape=(block, block, scale, scale),
            in_specs=[held] * 4 + [vmem],
            out_specs=(vmem,) * 4,
            scratch_shapes=[
                pltpu.VMEM((2, rows, columns), jnp.float32),
                pltpu.VMEM((2, rows, columns), jnp.float32),
                pltpu.VMEM((rows, LANES), jnp.float32),
                pltpu.VMEM((2, count, 1, columns), jnp.float32),
                dma(4 * pieces), dma(2 * count - 2), dma(2 * count - 2),
                dma(line), dma(line), dma(line), dma(line), dma(wide), dma(wide), dma(pieces), dma(pieces),
            ],
            compiler_params=pltpu.CompilerParams(
                collective_id=0, has_side_effects=True,
                vmem_limit_bytes=VMEM_BYTES - 2 * full[0] * full[1] * 2 - (1 << 19),
            ),
        )(train_gate, slow_gate, train_up, slow_up, norm_gain[None, :])
        parts = 4
        return pl.pallas_call(
            functools.partial(store_kernel, parts),
            out_shape=(jax.ShapeDtypeStruct(full, jnp.bfloat16),) * 2 + (jax.ShapeDtypeStruct((columns,), jnp.float32),) * 2,
            in_specs=[vmem] * 4,
            out_specs=(held,) * 4,
            scratch_shapes=[dma(2 * parts + 2)],
            compiler_params=pltpu.CompilerParams(vmem_limit_bytes=1 << 20),
        )(*gathered)

    in_specs = (P("zero", "tp"), P("zero", "tp"), P("zero", "tp"), P("zero", "tp"), P("zero"))
    out_specs = (P(None, "tp"), P(None, "tp"), P("tp"), P("tp"))
    return jax.shard_map(body, mesh=mesh, in_specs=in_specs, out_specs=out_specs, check_vma=False)
```

```python
import functools

import jax
import jax.numpy as jnp
from jax import lax
from jax.experimental import pallas as pl
from jax.experimental.pallas import tpu as pltpu
from jax.sharding import PartitionSpec as P

keep_rate = 0.75
MESH = pl.DeviceIdType.MESH
SIDE = 2
LANES = 128
GROUP = 8
VMEM_BYTES = 67_043_328


def gather_kernel(
    count, pieces,
    train_gate, slow_gate, train_up, slow_up, gain_ref,
    gate_ref, up_ref, scale_gate_ref, scale_up_ref,
    train, slow, gains, sums,
    load_sem, sum_send, sum_recv,
    left_send, left_recv, right_send, right_recv, side_send, side_recv, half_send, half_recv,
):
    length = count // SIDE
    rows, columns = train_gate.shape
    piece_rows = rows // pieces
    me = lax.axis_index("zero")
    place, side = me // SIDE, me % SIDE
    outs = (gate_ref, up_ref)
    scales = (scale_gate_ref, scale_up_ref)

    barrier = pltpu.get_barrier_semaphore()
    for step in range(1, count):
        pl.semaphore_signal(barrier, 1, device_id={"zero": lax.rem(me + step, count)}, device_id_type=MESH)

    loads = []
    for which, (t, s) in enumerate(((train_gate, slow_gate), (train_up, slow_up))):
        for p in range(pieces):
            at = pl.ds(p * piece_rows, piece_rows)
            k = (which * pieces + p) * 2
            loads.append((
                pltpu.make_async_copy(t.at[at], train.at[which, at], load_sem.at[k]),
                pltpu.make_async_copy(s.at[at], slow.at[which, at], load_sem.at[k + 1]),
            ))
    for pair in loads:
        for load in pair:
            load.start()

    gains[...] = jnp.broadcast_to(gain_ref[...], (LANES, rows)).T

    def sum_copy(which, step, source, to):
        k = which * (count - 1) + step - 1
        return pltpu.make_async_remote_copy(
            src_ref=sums.at[which, source], dst_ref=sums.at[which, source],
            send_sem=sum_send.at[k], recv_sem=sum_recv.at[k],
            device_id={"zero": to}, device_id_type=MESH,
        )

    for which in range(2):
        def add(i, total):
            at = pl.ds(pl.multiple_of(i * GROUP, GROUP), GROUP)
            gain = jnp.concatenate([gains[at, :]] * (columns // LANES), axis=1)
            gained = (keep_rate * slow[which, at, :] + (1.0 - keep_rate) * train[which, at, :]) * gain
            slow[which, at, :] = gained
            return total + gained * gained

        total = jnp.zeros((GROUP, columns), jnp.float32)
        for p in range(pieces):
            for load in loads[which * pieces + p]:
                load.wait()
            total = lax.fori_loop(p * piece_rows // GROUP, (p + 1) * piece_rows // GROUP, add, total)
        sums[which, me] = jnp.sum(total, axis=0, keepdims=True)
        if which == 0:
            pl.semaphore_wait(barrier, count - 1)
        for step in range(1, count):
            sum_copy(which, step, me, lax.rem(me + step, count)).start()

    def part_of(owner_place, owner_side, which, p):
        start = (owner_place * SIDE + owner_side) * rows + p * piece_rows
        return outs[which].at[pl.ds(pl.multiple_of(start, piece_rows), piece_rows)]

    def copy_to(ref, send, recv, to):
        return pltpu.make_async_remote_copy(
            src_ref=ref, dst_ref=ref, send_sem=send, recv_sem=recv,
            device_id={"zero": to}, device_id_type=MESH,
        )

    to_left = jnp.maximum(place - 1, 0) * SIDE + side
    to_right = jnp.minimum(place + 1, length - 1) * SIDE + side
    to_side = place * SIDE + (SIDE - 1 - side)
    has_left, has_right = place > 0, place < length - 1
    is_even = place % 2 == 0
    twin = place + 1 - 2 * (place % 2)
    to_twin = twin * SIDE + side
    half_round = jnp.maximum(jnp.where(is_even, place, length - 1 - place), 1)
    order = [(which, p) for which in range(2) for p in range(pieces)]

    def left_copy(distance, which, p):
        k = distance * 2 * pieces + which * pieces + p
        return copy_to(part_of(place + distance, side, which, p), left_send.at[k], left_recv.at[k], to_left)

    def right_copy(distance, which, p):
        k = distance * 2 * pieces + which * pieces + p
        return copy_to(part_of(place - distance, side, which, p), right_send.at[k], right_recv.at[k], to_right)

    def side_index(distance, which, p):
        d = distance if distance >= 0 else length - 1 - distance
        return d * 2 * pieces + which * pieces + p

    def side_copy(distance, which, p):
        k = side_index(distance, which, p)
        return copy_to(part_of(place + distance, side, which, p), side_send.at[k], side_recv.at[k], to_side)

    def side_arrival(distance, which, p):
        k = side_index(distance, which, p)
        return copy_to(part_of(place + distance, SIDE - 1 - side, which, p), side_send.at[k], side_recv.at[k], to_side)

    def half_copy(p):
        return copy_to(part_of(place, SIDE - 1 - side, 1, p), half_send.at[p], half_recv.at[p], to_twin)

    def half_arrival(p):
        return copy_to(part_of(twin, SIDE - 1 - side, 1, p), half_send.at[p], half_recv.at[p], to_twin)

    def in_line(distance):
        return place + distance <= length - 1 if distance > 0 else place + distance >= 0

    def by_side(distance, which):
        ok = in_line(distance)
        if which == 1 and distance == 1:
            ok = jnp.logical_and(ok, jnp.logical_not(is_even))
        if which == 1 and distance == -1:
            ok = jnp.logical_and(ok, is_even)
        return ok

    def send_own(which, p):
        @pl.when(has_left)
        def _():
            left_copy(0, which, p).start()

        @pl.when(has_right)
        def _():
            right_copy(0, which, p).start()

        side_copy(0, which, p).start()

    for which in range(2):
        for step in range(1, count):
            source = lax.rem(me + count - step, count)
            sum_copy(which, step, source, source).wait_recv()
        total = sums[which, 0]
        for k in range(1, count):
            total = total + sums[which, k]
        scale = jnp.sqrt(total)
        scales[which][...] = scale
        inverse = 1.0 / scale
        for p in range(pieces + 1):
            if p < pieces:
                at = pl.ds(p * piece_rows, piece_rows)
                start = pl.multiple_of(me * rows + p * piece_rows, piece_rows)
                outs[which][pl.ds(start, piece_rows), :] = (slow[which, at, :] * inverse).astype(jnp.bfloat16)
            if p > 0:
                send_own(which, p - 1)

    for k in range(1, length):
        for which, p in order:
            @pl.when(in_line(k))
            def _():
                q = (k - 1) * 2 * pieces + which * pieces + p
                copy_to(part_of(place + k, side, which, p), left_send.at[q], left_recv.at[q], to_right).wait_recv()

                @pl.when(has_left)
                def _():
                    left_copy(k, which, p).start()

            @pl.when(by_side(k, which))
            def _():
                side_copy(k, which, p).start()

            @pl.when(in_line(-k))
            def _():
                q = (k - 1) * 2 * pieces + which * pieces + p
                copy_to(part_of(place - k, side, which, p), right_send.at[q], right_recv.at[q], to_left).wait_recv()

                @pl.when(has_right)
                def _():
                    right_copy(k, which, p).start()

            @pl.when(by_side(-k, which))
            def _():
                side_copy(-k, which, p).start()

        @pl.when(half_round == k)
        def _():
            for p in range(pieces):
                side_arrival(0, 1, p).wait_recv()
                half_copy(p).start()

    for p in range(pieces):
        side_arrival(0, 0, p).wait_recv()

    for k in range(1, length):
        for which, p in order:
            for distance in (k, -k):
                @pl.when(by_side(distance, which))
                def _():
                    side_arrival(distance, which, p).wait_recv()
                    side_copy(distance, which, p).wait_send()

    for p in range(pieces):
        half_arrival(p).wait_recv()
        half_copy(p).wait_send()

    for which in range(2):
        for step in range(1, count):
            sum_copy(which, step, me, lax.rem(me + step, count)).wait_send()
    for which, p in order:
        side_copy(0, which, p).wait_send()
        for k in range(length):
            @pl.when(jnp.logical_and(has_left, place + k <= length - 1))
            def _():
                left_copy(k, which, p).wait_send()

            @pl.when(jnp.logical_and(has_right, place - k >= 0))
            def _():
                right_copy(k, which, p).wait_send()


def store_kernel(parts, gate, up, scale_gate, scale_up, gate_out, up_out, scale_gate_out, scale_up_out, sem):
    rows = gate.shape[0] // parts
    copies = []
    for which, (held, out) in enumerate(((gate, gate_out), (up, up_out))):
        for k in range(parts):
            at = pl.ds(k * rows, rows)
            copies.append(pltpu.make_async_copy(held.at[at], out.at[at], sem.at[which * parts + k]))
    copies.append(pltpu.make_async_copy(scale_gate.at[0], scale_gate_out, sem.at[2 * parts]))
    copies.append(pltpu.make_async_copy(scale_up.at[0], scale_up_out, sem.at[2 * parts + 1]))
    for copy in copies:
        copy.start()
    for copy in copies:
        copy.wait()


def solution(mesh):
    count = mesh.shape["zero"]

    def body(train_gate, slow_gate, train_up, slow_up, norm_gain):
        rows, columns = train_gate.shape
        pieces = max(1, min(2, rows // 64))
        length = count // SIDE
        full = (rows * count, columns)
        block = pltpu.VMEM(full, jnp.bfloat16)
        scale = pltpu.VMEM((1, columns), jnp.float32)
        vmem, held = pl.BlockSpec(memory_space=pltpu.VMEM), pl.BlockSpec(memory_space=pltpu.HBM)
        dma = lambda n: pltpu.SemaphoreType.DMA((n,))
        line, wide = length * 2 * pieces, (2 * length - 1) * 2 * pieces
        gathered = pl.pallas_call(
            functools.partial(gather_kernel, count, pieces),
            out_shape=(block, block, scale, scale),
            in_specs=[held] * 4 + [vmem],
            out_specs=(vmem,) * 4,
            scratch_shapes=[
                pltpu.VMEM((2, rows, columns), jnp.float32),
                pltpu.VMEM((2, rows, columns), jnp.float32),
                pltpu.VMEM((rows, LANES), jnp.float32),
                pltpu.VMEM((2, count, 1, columns), jnp.float32),
                dma(4 * pieces), dma(2 * count - 2), dma(2 * count - 2),
                dma(line), dma(line), dma(line), dma(line), dma(wide), dma(wide), dma(pieces), dma(pieces),
            ],
            compiler_params=pltpu.CompilerParams(
                collective_id=0, has_side_effects=True,
                vmem_limit_bytes=VMEM_BYTES - 2 * full[0] * full[1] * 2 - (1 << 19),
            ),
        )(train_gate, slow_gate, train_up, slow_up, norm_gain[None, :])
        parts = 4
        return pl.pallas_call(
            functools.partial(store_kernel, parts),
            out_shape=(jax.ShapeDtypeStruct(full, jnp.bfloat16),) * 2 + (jax.ShapeDtypeStruct((columns,), jnp.float32),) * 2,
            in_specs=[vmem] * 4,
            out_specs=(held,) * 4,
            scratch_shapes=[dma(2 * parts + 2)],
            compiler_params=pltpu.CompilerParams(vmem_limit_bytes=1 << 20),
        )(*gathered)

    in_specs = (P("zero", "tp"), P("zero", "tp"), P("zero", "tp"), P("zero", "tp"), P("zero"))
    out_specs = (P(None, "tp"), P(None, "tp"), P("tp"), P("tp"))
    return jax.shard_map(body, mesh=mesh, in_specs=in_specs, out_specs=out_specs, check_vma=False)
```

```python
import functools

import jax
import jax.numpy as jnp
from jax import lax
from jax.experimental import pallas as pl
from jax.experimental.pallas import tpu as pltpu
from jax.sharding import PartitionSpec as P

keep_rate = 0.75
MESH = pl.DeviceIdType.MESH
SIDE = 2
LANES = 128
GROUP = 8
HEAD = 16
LEAD = 16
VMEM_BYTES = 67_043_328


def gather_kernel(
    count, pieces, head,
    train_gate, slow_gate, train_up, slow_up, gain_ref,
    gate_ref, up_ref, scale_gate_ref, scale_up_ref,
    train, slow, gains, sums, heads,
    head_send, head_recv, load_sem, sum_send, sum_recv,
    left_send, left_recv, right_send, right_recv, side_send, side_recv, half_send, half_recv,
):
    length = count // SIDE
    rows, columns = train_gate.shape
    piece_rows = rows // pieces
    me = lax.axis_index("zero")
    place, side = me // SIDE, me % SIDE
    outs = (gate_ref, up_ref)
    scales = (scale_gate_ref, scale_up_ref)

    barrier = pltpu.get_barrier_semaphore()
    for step in range(1, count):
        pl.semaphore_signal(barrier, 1, device_id={"zero": lax.rem(me + step, count)}, device_id_type=MESH)

    loads = []
    for which, (t, s) in enumerate(((train_gate, slow_gate), (train_up, slow_up))):
        for p in range(pieces):
            at = pl.ds(p * piece_rows, piece_rows)
            k = (which * pieces + p) * 2
            loads.append((
                pltpu.make_async_copy(t.at[at], train.at[which, at], load_sem.at[k]),
                pltpu.make_async_copy(s.at[at], slow.at[which, at], load_sem.at[k + 1]),
            ))
    for pair in loads:
        for load in pair:
            load.start()

    gains[...] = jnp.broadcast_to(gain_ref[...], (LANES, rows)).T

    def sum_copy(which, step, source, to):
        k = which * (count - 1) + step - 1
        return pltpu.make_async_remote_copy(
            src_ref=sums.at[which, source], dst_ref=sums.at[which, source],
            send_sem=sum_send.at[k], recv_sem=sum_recv.at[k],
            device_id={"zero": to}, device_id_type=MESH,
        )

    to_left = jnp.maximum(place - 1, 0) * SIDE + side
    to_right = jnp.minimum(place + 1, length - 1) * SIDE + side
    to_side = place * SIDE + (SIDE - 1 - side)
    has_left, has_right = place > 0, place < length - 1
    for which in range(2):
        def add(i, total):
            at = pl.ds(pl.multiple_of(i * GROUP, GROUP), GROUP)
            gain = jnp.concatenate([gains[at, :]] * (columns // LANES), axis=1)
            gained = (keep_rate * slow[which, at, :] + (1.0 - keep_rate) * train[which, at, :]) * gain
            slow[which, at, :] = gained
            return total + gained * gained

        total = jnp.zeros((GROUP, columns), jnp.float32)
        for p in range(pieces):
            for load in loads[which * pieces + p]:
                load.wait()
            total = lax.fori_loop(p * piece_rows // GROUP, (p + 1) * piece_rows // GROUP, add, total)
        sums[which, me] = jnp.sum(total, axis=0, keepdims=True)
        if which == 0:
            pl.semaphore_wait(barrier, count - 1)
        for step in range(1, count):
            sum_copy(which, step, me, lax.rem(me + step, count)).start()

    def head_copy(slot, to):
        return pltpu.make_async_remote_copy(
            src_ref=slow.at[0, pl.ds(0, head)], dst_ref=heads.at[slot],
            send_sem=head_send.at[slot], recv_sem=head_recv.at[slot],
            device_id={"zero": to}, device_id_type=MESH,
        )

    @pl.when(has_left)
    def _():
        head_copy(0, to_left).start()

    @pl.when(has_right)
    def _():
        head_copy(1, to_right).start()

    head_copy(2, to_side).start()

    def part_of(owner_place, owner_side, which, p, skip=0):
        start = (owner_place * SIDE + owner_side) * rows + p * piece_rows + skip
        step = GROUP * 2 if skip else piece_rows
        return outs[which].at[pl.ds(pl.multiple_of(start, step), piece_rows - skip)]

    def skipped(distance, which, p):
        return head if (distance, which, p) == (0, 0, 0) else 0

    def copy_to(ref, send, recv, to):
        return pltpu.make_async_remote_copy(
            src_ref=ref, dst_ref=ref, send_sem=send, recv_sem=recv,
            device_id={"zero": to}, device_id_type=MESH,
        )

    is_even = place % 2 == 0
    twin = place + 1 - 2 * (place % 2)
    to_twin = twin * SIDE + side
    half_round = jnp.maximum(jnp.where(is_even, place, length - 1 - place), 1)
    order = [(which, p) for which in range(2) for p in range(pieces)]

    def left_copy(distance, which, p):
        k = distance * 2 * pieces + which * pieces + p
        return copy_to(part_of(place + distance, side, which, p, skipped(distance, which, p)), left_send.at[k], left_recv.at[k], to_left)

    def right_copy(distance, which, p):
        k = distance * 2 * pieces + which * pieces + p
        return copy_to(part_of(place - distance, side, which, p, skipped(distance, which, p)), right_send.at[k], right_recv.at[k], to_right)

    def side_index(distance, which, p):
        d = distance if distance >= 0 else length - 1 - distance
        return d * 2 * pieces + which * pieces + p

    def side_copy(distance, which, p):
        k = side_index(distance, which, p)
        return copy_to(part_of(place + distance, side, which, p, skipped(distance, which, p)), side_send.at[k], side_recv.at[k], to_side)

    def side_arrival(distance, which, p):
        k = side_index(distance, which, p)
        return copy_to(part_of(place + distance, SIDE - 1 - side, which, p, skipped(distance, which, p)), side_send.at[k], side_recv.at[k], to_side)

    def half_copy(p):
        return copy_to(part_of(place, SIDE - 1 - side, 1, p), half_send.at[p], half_recv.at[p], to_twin)

    def half_arrival(p):
        return copy_to(part_of(twin, SIDE - 1 - side, 1, p), half_send.at[p], half_recv.at[p], to_twin)

    def in_line(distance):
        return place + distance <= length - 1 if distance > 0 else place + distance >= 0

    def by_side(distance, which):
        ok = in_line(distance)
        if which == 1 and distance == 1:
            ok = jnp.logical_and(ok, jnp.logical_not(is_even))
        if which == 1 and distance == -1:
            ok = jnp.logical_and(ok, is_even)
        return ok

    def send_own(which, p):
        @pl.when(has_left)
        def _():
            left_copy(0, which, p).start()

        @pl.when(has_right)
        def _():
            right_copy(0, which, p).start()

        side_copy(0, which, p).start()

    for which in range(2):
        for step in range(1, count):
            source = lax.rem(me + count - step, count)
            sum_copy(which, step, source, source).wait_recv()
        total = sums[which, 0]
        for k in range(1, count):
            total = total + sums[which, k]
        scale = jnp.sqrt(total)
        scales[which][...] = scale
        inverse = 1.0 / scale
        def store(p, first, size):
            start = pl.multiple_of(me * rows + p * piece_rows + first, GROUP * 2)
            block = slow[which, pl.ds(p * piece_rows + first, size), :]
            outs[which][pl.ds(start, size), :] = (block * inverse).astype(jnp.bfloat16)

        for p in range(pieces + 1):
            if p < pieces:
                store(p, 0, LEAD)
            if p > 0:
                send_own(which, p - 1)
            if p < pieces:
                store(p, LEAD, piece_rows - LEAD)

        if which == 0:
            def use_head(slot, owner, sender):
                head_copy(slot, sender).wait_recv()
                start = pl.multiple_of(owner * rows, GROUP * 2)
                outs[0][pl.ds(start, head), :] = (heads[slot] * inverse).astype(jnp.bfloat16)

            @pl.when(has_right)
            def _():
                use_head(0, to_right, to_right)

            @pl.when(has_left)
            def _():
                use_head(1, to_left, to_left)

            use_head(2, to_side, to_side)

    for k in range(1, length):
        for which, p in order:
            @pl.when(in_line(k))
            def _():
                q = (k - 1) * 2 * pieces + which * pieces + p
                copy_to(part_of(place + k, side, which, p, skipped(k - 1, which, p)), left_send.at[q], left_recv.at[q], to_right).wait_recv()

                @pl.when(has_left)
                def _():
                    left_copy(k, which, p).start()

            @pl.when(by_side(k, which))
            def _():
                side_copy(k, which, p).start()

            @pl.when(in_line(-k))
            def _():
                q = (k - 1) * 2 * pieces + which * pieces + p
                copy_to(part_of(place - k, side, which, p, skipped(k - 1, which, p)), right_send.at[q], right_recv.at[q], to_left).wait_recv()

                @pl.when(has_right)
                def _():
                    right_copy(k, which, p).start()

            @pl.when(by_side(-k, which))
            def _():
                side_copy(-k, which, p).start()

        @pl.when(half_round == k)
        def _():
            for p in range(pieces):
                side_arrival(0, 1, p).wait_recv()
                half_copy(p).start()

    for p in range(pieces):
        side_arrival(0, 0, p).wait_recv()

    for k in range(1, length):
        for which, p in order:
            for distance in (k, -k):
                @pl.when(by_side(distance, which))
                def _():
                    side_arrival(distance, which, p).wait_recv()
                    side_copy(distance, which, p).wait_send()

    for p in range(pieces):
        half_arrival(p).wait_recv()
        half_copy(p).wait_send()

    for which in range(2):
        for step in range(1, count):
            sum_copy(which, step, me, lax.rem(me + step, count)).wait_send()

    @pl.when(has_left)
    def _():
        head_copy(0, to_left).wait_send()

    @pl.when(has_right)
    def _():
        head_copy(1, to_right).wait_send()

    head_copy(2, to_side).wait_send()
    for which, p in order:
        side_copy(0, which, p).wait_send()
        for k in range(length):
            @pl.when(jnp.logical_and(has_left, place + k <= length - 1))
            def _():
                left_copy(k, which, p).wait_send()

            @pl.when(jnp.logical_and(has_right, place - k >= 0))
            def _():
                right_copy(k, which, p).wait_send()


def store_kernel(parts, gate, up, scale_gate, scale_up, gate_out, up_out, scale_gate_out, scale_up_out, sem):
    rows = gate.shape[0] // parts
    copies = []
    for which, (held, out) in enumerate(((gate, gate_out), (up, up_out))):
        for k in range(parts):
            at = pl.ds(k * rows, rows)
            copies.append(pltpu.make_async_copy(held.at[at], out.at[at], sem.at[which * parts + k]))
    copies.append(pltpu.make_async_copy(scale_gate.at[0], scale_gate_out, sem.at[2 * parts]))
    copies.append(pltpu.make_async_copy(scale_up.at[0], scale_up_out, sem.at[2 * parts + 1]))
    for copy in copies:
        copy.start()
    for copy in copies:
        copy.wait()


def solution(mesh):
    count = mesh.shape["zero"]

    def body(train_gate, slow_gate, train_up, slow_up, norm_gain):
        rows, columns = train_gate.shape
        pieces = max(1, min(2, rows // 64))
        head = HEAD
        length = count // SIDE
        full = (rows * count, columns)
        block = pltpu.VMEM(full, jnp.bfloat16)
        scale = pltpu.VMEM((1, columns), jnp.float32)
        vmem, held = pl.BlockSpec(memory_space=pltpu.VMEM), pl.BlockSpec(memory_space=pltpu.HBM)
        dma = lambda n: pltpu.SemaphoreType.DMA((n,))
        line, wide = length * 2 * pieces, (2 * length - 1) * 2 * pieces
        gathered = pl.pallas_call(
            functools.partial(gather_kernel, count, pieces, head),
            out_shape=(block, block, scale, scale),
            in_specs=[held] * 4 + [vmem],
            out_specs=(vmem,) * 4,
            scratch_shapes=[
                pltpu.VMEM((2, rows, columns), jnp.float32),
                pltpu.VMEM((2, rows, columns), jnp.float32),
                pltpu.VMEM((rows, LANES), jnp.float32),
                pltpu.VMEM((2, count, 1, columns), jnp.float32),
                pltpu.VMEM((3, head, columns), jnp.float32),
                dma(3), dma(3), dma(4 * pieces), dma(2 * count - 2), dma(2 * count - 2),
                dma(line), dma(line), dma(line), dma(line), dma(wide), dma(wide), dma(pieces), dma(pieces),
            ],
            compiler_params=pltpu.CompilerParams(
                collective_id=0, has_side_effects=True,
                vmem_limit_bytes=VMEM_BYTES - 2 * full[0] * full[1] * 2 - (1 << 19),
            ),
        )(train_gate, slow_gate, train_up, slow_up, norm_gain[None, :])
        parts = 4
        return pl.pallas_call(
            functools.partial(store_kernel, parts),
            out_shape=(jax.ShapeDtypeStruct(full, jnp.bfloat16),) * 2 + (jax.ShapeDtypeStruct((columns,), jnp.float32),) * 2,
            in_specs=[vmem] * 4,
            out_specs=(held,) * 4,
            scratch_shapes=[dma(2 * parts + 2)],
            compiler_params=pltpu.CompilerParams(vmem_limit_bytes=1 << 20),
        )(*gathered)

    in_specs = (P("zero", "tp"), P("zero", "tp"), P("zero", "tp"), P("zero", "tp"), P("zero"))
    out_specs = (P(None, "tp"), P(None, "tp"), P("tp"), P("tp"))
    return jax.shard_map(body, mesh=mesh, in_specs=in_specs, out_specs=out_specs, check_vma=False)
```
